256 devices in a mesh: ctx: 64 (over z, x_hi, y), tp: 4 (over x_lo, core).
Axes of the slice: x: 4 (x_hi: 2, x_lo: 2; x = x_hi * 2 + x_lo), y: 4, z: 8, core: 2. Of those that a mesh axis runs over, the one named last changes fastest.
Arguments:
- queries: bfloat16 [32768, 4096], P('ctx', 'tp'), may hold values from -22 to 22
- keys: bfloat16 [32768, 512], P('ctx', 'tp'), may hold values from -22 to 22
- values: bfloat16 [32768, 512], P('ctx', 'tp'), may hold values from -36 to 36
- positions: int32 [3, 32768], P(None, 'ctx'), may hold values from 0 to 32767
- segment_ids: int32 [32768], replicated, may hold values from 0 to 31, never falling along the last dimension, each value on 1 to 2048 neighbouring positions
- out_weight: bfloat16 [4096, 8192], P('tp', 'ctx'), may hold values from -0.09375 to 0.09375
- residual: bfloat16 [32768, 8192], P(('ctx', 'tp')), may hold values from -3 to 3
Outputs:
- layer_out: bfloat16 [32768, 8192], P(('ctx', 'tp'))
The draws below stay inside these ranges and needn't reach their ends.
Inputs may be any that keep to these rules, and one draw needn't show every extreme that they name: `segment_ids`: ids never fall along the sequence; each document has 1 to 2048 tokens, and one has exactly 2048.
All inputs are finite; a program needn't handle non-finite values.
Results may differ from the reference program's by a relative error of at most 0.013.
Values may be sent and summed in bfloat16 or wider, within the bound.
No kernel may reach another device: no remote copies, remote signals or barrier semaphores. Data moves between devices by JAX's collectives and lax.ppermute only.
A program may use at most 128 MiB of HBM per device.

```python
import math
import jax
import jax.numpy as jnp
import numpy as np
from jax import lax

D = 8192
HD = 128
HQ = 32
HK = 4
DOC = 2048
SEQ = 32768
DOCS = 32
N_TP = 4


def drawn_rows(key, row_count, col_count):
    base_key = jax.random.fold_in(key, 0)
    return jnp.clip(jax.random.normal(base_key, (row_count, col_count), jnp.float32), -6.0, 6.0)


def draw_queries(key, part):
    return drawn_rows(jax.random.fold_in(key, 11), SEQ, HQ * HD).astype(jnp.bfloat16)


def draw_keys(key, part):
    return drawn_rows(jax.random.fold_in(key, 23), SEQ, HK * HD).astype(jnp.bfloat16)


def plant(drawn, stream_key, least, largest):
    index_at = [jax.random.randint(jax.random.fold_in(stream_key, axis), (), 0, length) for axis, length in enumerate(drawn.shape)]
    main_axis = drawn.shape.index(max(drawn.shape))
    beside = index_at[:main_axis] + [(index_at[main_axis] + 1) % drawn.shape[main_axis]] + index_at[main_axis + 1:]
    return drawn.at[tuple(index_at)].set(least).at[tuple(beside)].set(largest)


def levels(key, extent, cuts, least, largest):
    gain = 1.0
    for dim, parts in cuts:
        steps = jax.random.uniform(jax.random.fold_in(jax.random.fold_in(key, 6), dim), (parts,), jnp.float32, least / len(cuts), largest / len(cuts))
        gain = gain * jnp.repeat(jnp.exp(steps), extent[dim] // parts).reshape((-1,) + (1,) * (len(extent) - 1 - dim))
    return gain


def length_profile(count, total, reach, lean):
    portions = [(1 << 20) // math.isqrt(grade ** lean) + 1 for grade in range(2, count + 1)]
    surplus, counts = total - reach - (count - 1), [1] * (count - 1)
    while surplus > 0:
        movable = [i for i in range(count - 1) if counts[i] < reach]
        mass, remaining = sum([portions[i] for i in movable]), surplus
        for i in movable:
            extra = min(reach - counts[i], max(1, remaining * portions[i] // mass), surplus)
            counts[i] = counts[i] + extra
            surplus = surplus - extra
    return np.array([reach] + counts)


def uneven(stream_key, number_of, total, bound, skew):
    if number_of == 2:
        one = jax.random.randint(stream_key, (), max(1, total - bound), min(bound, total - 1) + 1)
        return jnp.stack([one, total - one])
    sizes = jnp.asarray(length_profile(number_of, total, bound, skew), jnp.int32)
    couples = (number_of - 1) // 2
    source_of, receiver = sizes[1:1 + 2 * couples:2], sizes[2:2 + 2 * couples:2]
    margin = jnp.minimum(source_of - 1, bound - receiver)
    moved = jax.random.randint(jax.random.fold_in(stream_key, 1), (couples,), 0, 1 << 20) % (margin + 1)
    sizes = sizes.at[1:1 + 2 * couples:2].set(source_of - moved).at[2:2 + 2 * couples:2].set(receiver + moved)
    return sizes[jax.random.permutation(jax.random.fold_in(stream_key, 2), number_of)]


def noise(stream_key, shape, scale, limit, shards=(), kind=jnp.bfloat16):
    array = jax.random.normal(stream_key, shape, jnp.float32) * scale
    if len(shards) > 0:
        array = levels(stream_key, shape, shards, -0.22, 0.18) * array
    return jnp.clip(array, min=-limit, max=limit).astype(kind)


def setup_inputs(seed: int = 0) -> dict:
    seeds = jax.random.split(jax.random.key(seed), 8)
    return {
        "queries": draw_queries(jax.random.fold_in(seeds[7], 71), 0),
        "keys": draw_keys(jax.random.fold_in(seeds[7], 71), 0),
        "values": noise(seeds[2], (SEQ, HK * HD), 6.0, 36.0, ((0, 64), (1, 4))),
        "positions": plant(jax.random.randint(seeds[3], (3, SEQ), 0, SEQ), jax.random.fold_in(seeds[3], 1), 0, SEQ - 1).astype(jnp.int32),
        "segment_ids": jnp.searchsorted(jnp.cumsum(uneven(seeds[4], DOCS, SEQ, DOC, 1)), jnp.arange(SEQ), side="right").astype(jnp.int32),
        "out_weight": noise(seeds[5], (HQ * HD, D), (HQ * HD) ** -0.5, 0.09375, ((0, 4), (1, 64))),
        "residual": noise(seeds[6], (SEQ, D), 0.5, 3.0, ((0, 256),)),
    }


theta_base = 1000000.0

def rotary_tables(positions):
    half_dim = HD // 2
    freq_index = jnp.arange(half_dim)
    inv_freq = theta_base ** (-2.0 * freq_index.astype(jnp.float32) / HD)
    first_end = HD // 8
    second_end = first_end + 3 * HD // 16
    place = positions.astype(jnp.float32)
    chosen = jnp.where(freq_index[None, :] < first_end, place[0][:, None], jnp.where(freq_index[None, :] < second_end, place[1][:, None], place[2][:, None]))
    angle = chosen * inv_freq[None, :]
    return (jnp.cos(angle), jnp.sin(angle))

def rotate(vectors, cosine_table, sine_table):
    half_dim = HD // 2
    lower_half = vectors[..., :half_dim]
    upper_half = vectors[..., half_dim:]
    cos_b = cosine_table[:, None, :]
    sin_b = sine_table[:, None, :]
    return jnp.concatenate([lower_half * cos_b - upper_half * sin_b, upper_half * cos_b + lower_half * sin_b], axis=-1)

def reference(queries, keys, values, positions, segment_ids, out_weight, residual):
    seq_len = queries.shape[0]
    group_size = HQ // HK
    cosine_table, sine_table = rotary_tables(positions)
    rot_q = rotate(queries.reshape(seq_len, HQ, HD).astype(jnp.float32), cosine_table, sine_table).astype(jnp.bfloat16)
    rot_k = rotate(keys.reshape(seq_len, HK, HD).astype(jnp.float32), cosine_table, sine_table).astype(jnp.bfloat16)
    key_heads = rot_k.transpose(1, 0, 2)
    value_heads = values.reshape(seq_len, HK, HD).transpose(1, 0, 2)
    query_rows = math.gcd(seq_len, 512)
    key_span = min(seq_len, DOC + query_rows)
    score_scale = 1.0 / math.sqrt(HD)

    def one_block(block_index):
        begin = (block_index * query_rows).astype(jnp.int32)
        key_start = jnp.clip(begin + query_rows - key_span, 0, seq_len - key_span).astype(jnp.int32)
        query_block = lax.dynamic_slice_in_dim(rot_q, begin, query_rows, 0)
        query_index = begin + jnp.arange(query_rows, dtype=jnp.int32)
        key_index = key_start + jnp.arange(key_span, dtype=jnp.int32)
        query_seg = lax.dynamic_slice_in_dim(segment_ids, begin, query_rows, 0)
        key_seg = lax.dynamic_slice_in_dim(segment_ids, key_start, key_span, 0)
        allowed = (key_index[None, :] <= query_index[:, None]) & (key_seg[None, :] == query_seg[:, None])
        grouped = query_block.reshape(query_rows, HK, group_size, HD).transpose(1, 0, 2, 3)
        key_part = lax.dynamic_slice_in_dim(key_heads, key_start, key_span, 1)
        value_part = lax.dynamic_slice_in_dim(value_heads, key_start, key_span, 1)

        def one_head(operands):
            query_head, key_head, value_head = operands
            score = jnp.einsum('qgd,nd->gqn', query_head.astype(jnp.float32), key_head.astype(jnp.float32)) * score_scale
            score = jnp.where(allowed[None], score, -1e+30)
            row_peak = lax.optimization_barrier(jnp.max(score, axis=-1, keepdims=True))
            prob = jnp.where(allowed[None], jnp.exp(score - row_peak), 0.0)
            row_sum = lax.optimization_barrier(jnp.sum(prob, axis=-1))
            mixed = jnp.einsum('gqn,nd->gqd', prob.astype(jnp.bfloat16).astype(jnp.float32), value_head.astype(jnp.float32))
            return (mixed / row_sum[..., None]).transpose(1, 0, 2)
        heads_out = lax.map(one_head, (grouped, key_part, value_part))
        return heads_out.transpose(1, 0, 2, 3).reshape(query_rows, HQ * HD)
    blocks = lax.map(one_block, jnp.arange(seq_len // query_rows, dtype=jnp.int32))
    attended = blocks.reshape(seq_len, HQ * HD).astype(jnp.bfloat16)
    part_cols = HQ * HD // N_TP
    summed = residual.astype(jnp.float32)
    for part_index in range(N_TP):
        cols = attended[:, part_index * part_cols:(part_index + 1) * part_cols]
        rows_w = out_weight[part_index * part_cols:(part_index + 1) * part_cols]
        partial_sum = jnp.dot(cols, rows_w, preferred_element_type=jnp.float32).astype(jnp.bfloat16)
        summed = summed + partial_sum.astype(jnp.float32)
    return summed.astype(jnp.bfloat16)
```

```python
import math

import jax
import jax.numpy as jnp
from jax import lax
from jax.experimental import pallas as pl
from jax.experimental.pallas import tpu as pltpu
from jax.sharding import Mesh, PartitionSpec as P

HD = 128
DOC = 2048
theta_base = 1000000.0

CTX = ("z", "xh", "y")
TP = ("xl", "c")
XRING = ("xh", "xl")

TOK = 512
HEADS = 8
TQ = 256
BACK = 4
NEG = -1e30
EXP2_SCALE = math.log2(math.e) / math.sqrt(HD)


def from_behind(block, distance):
    size = math.prod(lax.axis_size(a) for a in CTX)
    route = [(i - distance, i) for i in range(distance, size)]
    return lax.ppermute(block, CTX, route)


def rotary_tables(positions):
    half_dim = HD // 2
    freq_index = jnp.arange(half_dim)
    inv_freq = theta_base ** (-2.0 * freq_index.astype(jnp.float32) / HD)
    first_end = HD // 8
    second_end = first_end + 3 * HD // 16
    place = positions.astype(jnp.float32)
    chosen = jnp.where(
        freq_index[None, :] < first_end,
        place[0][:, None],
        jnp.where(freq_index[None, :] < second_end, place[1][:, None], place[2][:, None]),
    )
    angle = chosen * inv_freq[None, :]
    cosine, sine = jnp.cos(angle), jnp.sin(angle)
    return jnp.concatenate([cosine, cosine], 1), jnp.concatenate([-sine, sine], 1)


def dot_nt(a, b):
    return lax.dot_general(a, b, (((1,), (1,)), ((), ())), preferred_element_type=jnp.float32)


def values_and_ones(value):
    return jnp.concatenate([value, jnp.ones_like(value)], axis=1)


def first_step(h, rows, key, val, bias, rq_ref, m_ref, acc_ref):
    score = dot_nt(rq_ref[h, rows, :], key) + bias
    peak = jnp.max(score, axis=1, keepdims=True)
    prob = jnp.exp2((score - peak) * EXP2_SCALE)
    m_ref[h, rows, :] = jnp.broadcast_to(peak, (score.shape[0], HD))
    acc_ref[h, rows, :] = jnp.dot(prob.astype(jnp.bfloat16), val, preferred_element_type=jnp.float32)


def next_step(h, rows, key, val, bias, rq_ref, m_ref, acc_ref):
    score = dot_nt(rq_ref[h, rows, :], key) + bias
    old = m_ref[h, rows, :]
    new = jnp.maximum(old, jnp.broadcast_to(jnp.max(score, axis=1, keepdims=True), old.shape))
    keep = jnp.exp2((old - new) * EXP2_SCALE)
    wide = jnp.concatenate([new] * (score.shape[1] // HD), axis=1)
    prob = jnp.exp2((score - wide) * EXP2_SCALE)
    m_ref[h, rows, :] = new
    acc_ref[h, rows, :] = acc_ref[h, rows, :] * jnp.concatenate([keep, keep], axis=1) + jnp.dot(
        prob.astype(jnp.bfloat16), val, preferred_element_type=jnp.float32
    )


def own_kernel(seg_s, qseg_ref, kseg_ref, q_ref, cos_ref, sin_ref, kv_ref, rq_ref, m_ref, acc_ref):
    cosine, sine = cos_ref[...], sin_ref[...]
    for h in range(HEADS):
        x = q_ref[:, h * HD : (h + 1) * HD].astype(jnp.float32)
        rq_ref[h] = (x * cosine + pltpu.roll(x, HD // 2, 1) * sine).astype(jnp.bfloat16)
    base = BACK * TOK
    for i in range(TOK // TQ):
        rows = pl.ds(i * TQ, TQ)
        qseg = qseg_ref[rows, :]
        qseg = jnp.concatenate([qseg] * (TQ // HD), axis=1)
        row_id = lax.broadcasted_iota(jnp.int32, (TQ, TQ), 0)
        col_id = lax.broadcasted_iota(jnp.int32, (TQ, TQ), 1)
        kseg = kseg_ref[BACK : BACK + 1, i * TQ : (i + 1) * TQ]
        bias = jnp.where((qseg == kseg) & (col_id <= row_id), 0.0, NEG)
        key, val = kv_ref[rows, :HD], values_and_ones(kv_ref[rows, HD:])
        for h in range(HEADS):
            first_step(h, rows, key, val, bias, rq_ref, m_ref, acc_ref)
        for j in range(i):

            @pl.when(seg_s[base + j * TQ + TQ - 1] == seg_s[base + i * TQ])
            def _():
                cols = pl.ds(j * TQ, TQ)
                kseg = kseg_ref[BACK : BACK + 1, j * TQ : (j + 1) * TQ]
                bias = jnp.where(qseg == kseg, 0.0, NEG)
                key, val = kv_ref[cols, :HD], values_and_ones(kv_ref[cols, HD:])
                for h in range(HEADS):
                    next_step(h, rows, key, val, bias, rq_ref, m_ref, acc_ref)


def back_kernel(seg_s, qseg_ref, kseg_ref, rq_ref, m_in, acc_in, kv1, kv2, kv3, kv4, out_ref, m_ref, acc_ref, kv_ref):
    for d, block in enumerate((kv1, kv2, kv3, kv4)):
        kv_ref[BACK - 1 - d] = block[...]
    m_ref[...] = m_in[...]
    acc_ref[...] = acc_in[...]
    tiles = TOK // TQ

    def body(step, carry):
        b = step // tiles
        i = step % tiles
        q_first = pl.multiple_of(i * TQ, TQ)

        @pl.when(seg_s[b * TOK + TOK - 1] == seg_s[BACK * TOK + q_first])
        def _():
            rows = pl.ds(q_first, TQ)
            qseg = qseg_ref[rows, :]
            qseg = jnp.concatenate([qseg] * (TOK // HD), axis=1)
            bias = jnp.where(qseg == kseg_ref[pl.ds(b, 1), :], 0.0, NEG)
            key, val = kv_ref[b, :, :HD], values_and_ones(kv_ref[b, :, HD:])
            for h in range(HEADS):
                next_step(h, rows, key, val, bias, rq_ref, m_ref, acc_ref)

        return carry

    lax.fori_loop(0, BACK * tiles, body, 0)
    for h in range(HEADS):
        full = acc_ref[h]
        out_ref[:, h * HD : (h + 1) * HD] = (full[:, :HD] / full[:, HD:]).astype(jnp.bfloat16)


def attention(seg, qseg, kseg, queries, cosine, sine, kv, behind):
    smem = pl.BlockSpec(memory_space=pltpu.SMEM)
    vmem = pl.BlockSpec(memory_space=pltpu.VMEM)
    state = (
        jax.ShapeDtypeStruct((HEADS, TOK, HD), jnp.bfloat16),
        jax.ShapeDtypeStruct((HEADS, TOK, HD), jnp.float32),
        jax.ShapeDtypeStruct((HEADS, TOK, 2 * HD), jnp.float32),
    )
    rq, m, acc = pl.pallas_call(
        own_kernel,
        out_shape=state,
        in_specs=[smem] + [vmem] * 6,
        out_specs=(vmem,) * 3,
        compiler_params=pltpu.CompilerParams(vmem_limit_bytes=40 << 20),
        name="attend_own",
    )(seg, qseg, kseg, queries, cosine, sine, kv)
    return pl.pallas_call(
        back_kernel,
        out_shape=jax.ShapeDtypeStruct((TOK, HEADS * HD), jnp.bfloat16),
        in_specs=[smem] + [vmem] * 9,
        out_specs=vmem,
        scratch_shapes=[
            pltpu.VMEM((HEADS, TOK, HD), jnp.float32),
            pltpu.VMEM((HEADS, TOK, 2 * HD), jnp.float32),
            pltpu.VMEM((BACK, TOK, 2 * HD), jnp.bfloat16),
        ],
        compiler_params=pltpu.CompilerParams(vmem_limit_bytes=40 << 20),
        name="attend_back",
    )(seg, qseg, kseg, rq, m, acc, *behind)


def project_kernel(core, own_ref, oth_ref, w_ref, out_ref):
    acc = None
    for xl in range(2):
        for ref, which in ((own_ref, core[0]), (oth_ref, 1 - core[0])):
            t = 2 * xl + which
            w = jnp.concatenate([w_ref[0, t], w_ref[1, t]], axis=1)
            part = jnp.dot(ref[0, xl], w, preferred_element_type=jnp.float32)
            acc = part if acc is None else acc + part
    out_ref[...] = acc.astype(jnp.bfloat16)


def project(core, own, oth, weight):
    zs = weight.shape[0]
    return pl.pallas_call(
        project_kernel,
        out_shape=jax.ShapeDtypeStruct((2 * TOK, zs * HD), jnp.bfloat16),
        grid=(2, zs // 2),
        in_specs=[
            pl.BlockSpec(memory_space=pltpu.SMEM),
            pl.BlockSpec((1, 2, TOK, HEADS * HD), lambda s, n: (s, 0, 0, 0)),
            pl.BlockSpec((1, 2, TOK, HEADS * HD), lambda s, n: (s, 0, 0, 0)),
            pl.BlockSpec((2, 4, HEADS * HD, HD), lambda s, n: (n, 0, 0, 0)),
        ],
        out_specs=pl.BlockSpec((TOK, 2 * HD), lambda s, n: (s, n)),
        compiler_params=pltpu.CompilerParams(vmem_limit_bytes=48 << 20),
        name="project",
    )(core, own, oth, weight)


def finish_kernel(got_ref, res_ref, out_ref):
    srcs, zs = got_ref.shape[0], got_ref.shape[2] // HD
    for z in range(zs):
        for s in range(srcs):
            cols = pl.ds((z * srcs + s) * HD, HD)
            out_ref[:, cols] = (
                got_ref[s, :, z * HD : (z + 1) * HD].astype(jnp.float32)
                + res_ref[:, cols].astype(jnp.float32)
            ).astype(jnp.bfloat16)


def finish(got, residual):
    srcs, rows, cols = got.shape
    step = 32
    return pl.pallas_call(
        finish_kernel,
        out_shape=jax.ShapeDtypeStruct(residual.shape, jnp.bfloat16),
        grid=(rows // step,),
        in_specs=[
            pl.BlockSpec((srcs, step, cols), lambda r: (0, r, 0)),
            pl.BlockSpec((step, srcs * cols), lambda r: (r, 0)),
        ],
        out_specs=pl.BlockSpec((step, srcs * cols), lambda r: (r, 0)),
        name="finish",
    )(got, residual)


def on_device(queries, keys, values, positions, segment_ids, out_weight, residual):
    swap = [(y * 4 + t, t * 4 + y) for y in range(4) for t in range(4)]
    mine = lax.ppermute(out_weight, ("y",) + TP, swap)
    weight = lax.all_gather(mine, ("z", "y"), axis=0).reshape(8, 4, HEADS * HD, HD)

    cosine, sine = rotary_tables(positions)
    k32 = keys.astype(jnp.float32)
    flipped = jnp.concatenate([k32[:, HD // 2 :], k32[:, : HD // 2]], axis=1)
    rot_k = (k32 * cosine + flipped * sine).astype(jnp.bfloat16)
    kv = jnp.concatenate([rot_k, values], axis=1)
    behind = [from_behind(kv, d) for d in range(1, BACK + 1)]

    my_start = lax.axis_index(CTX) * TOK
    padded = jnp.concatenate([jnp.full((BACK * TOK,), -1, jnp.int32), segment_ids])
    seg = lax.dynamic_slice_in_dim(padded, my_start, (BACK + 1) * TOK, 0)
    qseg = jnp.broadcast_to(seg[BACK * TOK :, None], (TOK, HD))
    kseg = jnp.pad(seg.reshape(BACK + 1, TOK), ((0, 3), (0, 0)))
    attended = attention(seg, qseg, kseg, queries, cosine, sine, kv, behind)

    own = lax.all_to_all(jnp.broadcast_to(attended[None], (4,) + attended.shape), XRING, 0, 0)
    oth = lax.ppermute(own, "c", [(0, 1), (1, 0)])
    shape = (2, 2, TOK, HEADS * HD)
    core = lax.axis_index("c").astype(jnp.int32).reshape(1)
    out = project(core, own.reshape(shape), oth.reshape(shape), weight)
    got = lax.all_to_all(out.reshape(8, TOK // 4, out.shape[1]), XRING + ("c",), 0, 0)
    return finish(got, residual)


def solution(mesh):
    fine = Mesh(mesh.devices.reshape(8, 2, 4, 2, 2), CTX + TP)
    return jax.shard_map(
        on_device,
        mesh=fine,
        in_specs=(P(CTX, TP), P(CTX, TP), P(CTX, TP), P(None, CTX), P(), P(TP, CTX), P(CTX + TP, None)),
        out_specs=P(CTX + TP, None),
        check_vma=False,
    )
```

```python
import functools
import math

import jax
import jax.numpy as jnp
from jax import lax
from jax.experimental import pallas as pl
from jax.experimental.pallas import tpu as pltpu
from jax.sharding import Mesh, PartitionSpec as P


HD = 128
theta_base = 1000000.0

CTX = ("z", "xh", "y")
TP = ("xl", "c")
XRING = ("xh", "xl")

TOK = 512
HEADS = 8
PIECE = 64
CHUNKS = 2
TQ = TOK // CHUNKS
BACK = 4
NEG = -1e30
EXP2_SCALE = math.log2(math.e) / math.sqrt(HD)


def from_behind(block, distance):
    size = math.prod(lax.axis_size(a) for a in CTX)
    route = [(i - distance, i) for i in range(distance, size)]
    return lax.ppermute(block, CTX, route)


def rotary_tables(positions):
    half_dim = HD // 2
    freq_index = jnp.arange(half_dim)
    inv_freq = theta_base ** (-2.0 * freq_index.astype(jnp.float32) / HD)
    first_end = HD // 8
    second_end = first_end + 3 * HD // 16
    place = positions.astype(jnp.float32)
    chosen = jnp.where(
        freq_index[None, :] < first_end,
        place[0][:, None],
        jnp.where(freq_index[None, :] < second_end, place[1][:, None], place[2][:, None]),
    )
    angle = chosen * inv_freq[None, :]
    cosine, sine = jnp.cos(angle), jnp.sin(angle)
    return jnp.concatenate([cosine, cosine], 1), jnp.concatenate([-sine, sine], 1)


def dot_nt(a, b):
    return lax.dot_general(a, b, (((1,), (1,)), ((), ())), preferred_element_type=jnp.float32)


def values_and_ones(value):
    return jnp.concatenate([value, jnp.ones_like(value)], axis=1)


def first_step(h, key, val, bias, rq_ref, m_ref, acc_ref):
    score = dot_nt(rq_ref[h], key) + bias
    peak = jnp.max(score, axis=1, keepdims=True)
    prob = jnp.exp2((score - peak) * EXP2_SCALE)
    m_ref[h] = jnp.broadcast_to(peak, (score.shape[0], HD))
    acc_ref[h] = jnp.dot(prob.astype(jnp.bfloat16), val, preferred_element_type=jnp.float32)


def next_step(h, key, val, bias, rq_ref, m_ref, acc_ref):
    score = dot_nt(rq_ref[h], key) + bias
    old = m_ref[h]
    new = jnp.maximum(old, jnp.broadcast_to(jnp.max(score, axis=1, keepdims=True), old.shape))
    keep = jnp.exp2((old - new) * EXP2_SCALE)
    wide = jnp.concatenate([new] * (score.shape[1] // HD), axis=1)
    prob = jnp.exp2((score - wide) * EXP2_SCALE)
    m_ref[h] = new
    acc_ref[h] = acc_ref[h] * jnp.concatenate([keep, keep], axis=1) + jnp.dot(
        prob.astype(jnp.bfloat16), val, preferred_element_type=jnp.float32
    )


def chunk_rows(i):
    return [pl.ds(b * 2 * PIECE + i * PIECE, PIECE) for b in range(TOK // (2 * PIECE))]


SMEM = pl.BlockSpec(memory_space=pltpu.SMEM)


def whole(shape):
    return pl.BlockSpec(shape, lambda n: (0,) * len(shape))


def attend_kernel(i, seg_s, qseg_ref, kseg_ref, q_ref, cos_ref, sin_ref, kv0, kv1, kv2, kv3, kv4, out_ref, rq_ref, m_ref, acc_ref):
    rows = chunk_rows(i)
    cosine = jnp.concatenate([cos_ref[r, :] for r in rows], axis=0)
    sine = jnp.concatenate([sin_ref[r, :] for r in rows], axis=0)
    for h in range(HEADS):
        x = jnp.concatenate([q_ref[r, h * HD : (h + 1) * HD] for r in rows], axis=0)
        x = x.astype(jnp.float32)
        rq_ref[h] = (x * cosine + pltpu.roll(x, HD // 2, 1) * sine).astype(jnp.bfloat16)
    qseg = jnp.concatenate([qseg_ref[r, :] for r in rows], axis=0)
    qseg = jnp.concatenate([qseg] * (TOK // HD), axis=1)
    row = lax.broadcasted_iota(jnp.int32, (TQ, TOK), 0)
    col = lax.broadcasted_iota(jnp.int32, (TQ, TOK), 1)
    token = (row // PIECE) * (2 * PIECE) + i * PIECE + row % PIECE
    bias = jnp.where((qseg == kseg_ref[BACK : BACK + 1, :]) & (col <= token), 0.0, NEG)
    for h in range(HEADS):
        first_step(h, kv0[:, :HD], values_and_ones(kv0[:, HD:]), bias, rq_ref, m_ref, acc_ref)
    for b, kv in enumerate((kv4, kv3, kv2, kv1)):

        @pl.when(seg_s[b * TOK + TOK - 1] == seg_s[BACK * TOK + i * PIECE])
        def _():
            bias = jnp.where(qseg == kseg_ref[b : b + 1, :], 0.0, NEG)
            for h in range(HEADS):
                next_step(h, kv[:, :HD], values_and_ones(kv[:, HD:]), bias, rq_ref, m_ref, acc_ref)

    for h in range(HEADS):
        full = acc_ref[h]
        out_ref[:, h * HD : (h + 1) * HD] = (full[:, :HD] / full[:, HD:]).astype(jnp.bfloat16)


def attend(i, seg, *blocks):
    return pl.pallas_call(
        functools.partial(attend_kernel, i),
        out_shape=jax.ShapeDtypeStruct((TQ, HEADS * HD), jnp.bfloat16),
        grid=(1,),
        in_specs=[SMEM] + [whole(b.shape) for b in blocks],
        out_specs=whole((TQ, HEADS * HD)),
        scratch_shapes=[
            pltpu.VMEM((HEADS, TQ, HD), jnp.bfloat16),
            pltpu.VMEM((HEADS, TQ, HD), jnp.float32),
            pltpu.VMEM((HEADS, TQ, 2 * HD), jnp.float32),
        ],
        compiler_params=pltpu.CompilerParams(vmem_limit_bytes=24 << 20),
    )(seg, *blocks)


def project_kernel(at, own_ref, oth_ref, w_ref, out_ref):
    n = pl.program_id(0)

    def total(core_bit):
        acc = None
        for j in range(4):
            a = (own_ref, oth_ref)[(j & 1) ^ core_bit][(j >> 1) ^ at[1]]
            w = jnp.concatenate([w_ref[0, at[3] ^ j], w_ref[1, at[3] ^ j]], axis=1)
            part = jnp.dot(a, w, preferred_element_type=jnp.float32)
            acc = part if acc is None else acc + part
        cols = pl.ds(pl.multiple_of(n * 2 * HD, 2 * HD), 2 * HD)
        for e in range(2):
            for i in range(CHUNKS):
                first = (e * CHUNKS + i) * TQ
                block = acc[first : first + TQ].astype(jnp.bfloat16)
                s = at[0] if e == 0 else 1 - at[0]
                out_ref[s, :, i, :, cols] = block.reshape(TQ // PIECE, PIECE, 2 * HD)

    for bit in range(2):

        @pl.when(at[2] == bit)
        def _():
            total(bit)


def project(at, own, oth, weight):
    steps = weight.shape[0] // 2
    out = (2, TQ // PIECE, CHUNKS, PIECE, 2 * steps * HD)
    return pl.pallas_call(
        project_kernel,
        out_shape=jax.ShapeDtypeStruct(out, jnp.bfloat16),
        grid=(steps,),
        in_specs=[SMEM]
        + [pl.BlockSpec(memory_space=pltpu.VMEM)] * 2
        + [pl.BlockSpec((2,) + weight.shape[1:], lambda n: (n, 0, 0, 0))],
        out_specs=whole(out),
        compiler_params=pltpu.CompilerParams(vmem_limit_bytes=36 << 20),
        name="project",
    )(at, own, oth, weight)


def finish_kernel(got_ref, res_ref, out_ref):
    srcs, zs = got_ref.shape[0], got_ref.shape[2] // HD
    for z in range(zs):
        for s in range(srcs):
            cols = pl.ds((z * srcs + s) * HD, HD)
            out_ref[:, cols] = (
                got_ref[s, :, z * HD : (z + 1) * HD].astype(jnp.float32)
                + res_ref[:, cols].astype(jnp.float32)
            ).astype(jnp.bfloat16)


def finish(got, residual):
    srcs, rows, cols = got.shape
    step = 32
    wide = pl.BlockSpec((step, srcs * cols), lambda r: (r, 0))
    return pl.pallas_call(
        finish_kernel,
        out_shape=jax.ShapeDtypeStruct(residual.shape, jnp.bfloat16),
        grid=(rows // step,),
        in_specs=[pl.BlockSpec((srcs, step, cols), lambda r: (0, r, 0)), wide],
        out_specs=wide,
        compiler_params=pltpu.CompilerParams(vmem_limit_bytes=16 << 20),
        name="finish",
    )(got, residual)


def swap4(block, axes, j):
    return lax.ppermute(block, axes, [(r, r ^ j) for r in range(4)])


def gather4(i, block, axes):
    j1 = swap4(block, axes, 1)
    j3 = swap4(block, axes, 3)
    j2 = swap4(*((j3, axes, 1) if i == 0 else (j1, axes, 3)))
    return block, j1, j2, j3


def other_core(block):
    return lax.ppermute(block, "c", [(0, 1), (1, 0)])


def on_device(queries, keys, values, positions, segment_ids, out_weight, residual):
    swap = [(y * 4 + t, t * 4 + y) for y in range(4) for t in range(4)]
    mine = lax.ppermute(out_weight, ("y",) + TP, swap)
    weight = lax.all_gather(mine, ("z", "y"), axis=0).reshape((8, 4) + mine.shape)

    cosine, sine = rotary_tables(positions)
    k32 = keys.astype(jnp.float32)
    flipped = jnp.concatenate([k32[:, HD // 2 :], k32[:, : HD // 2]], axis=1)
    rot_k = (k32 * cosine + flipped * sine).astype(jnp.bfloat16)
    kv = jnp.concatenate([rot_k, values], axis=1)
    behind = [from_behind(kv, d) for d in range(1, BACK + 1)]

    my_start = lax.axis_index(CTX) * TOK
    padded = jnp.concatenate([jnp.full((BACK * TOK,), -1, jnp.int32), segment_ids])
    seg = lax.dynamic_slice_in_dim(padded, my_start, (BACK + 1) * TOK, 0)
    qseg = jnp.broadcast_to(seg[BACK * TOK :, None], (TOK, HD))
    kseg = jnp.pad(seg.reshape(BACK + 1, TOK), ((0, 3), (0, 0)))

    near, far = [[], []], [[], []]
    for i in range(CHUNKS):
        own = attend(i, seg, qseg, kseg, queries, cosine, sine, kv, *behind)
        own, j1, j2, j3 = gather4(i, own, XRING)
        for side, blocks in ((near, (own, j2)), (far, (j1, j3))):
            for rows, block in zip(side, blocks):
                rows.append(block)
    own = jnp.concatenate([b for side in (near, far) for rows in side for b in rows], axis=0)
    own = own.reshape(2, 2 * TOK, HEADS * HD)
    oth = other_core(own)

    xh, xl, c, y = (lax.axis_index(a).astype(jnp.int32) for a in ("xh", "xl", "c", "y"))
    at = jnp.stack([xh, (y >> 1) ^ xl, (y & 1) ^ c, y])
    out = project(at, own, oth, weight)
    out = out.reshape(8, CHUNKS * PIECE, out.shape[-1])
    got = lax.all_to_all(out, XRING + ("c",), 0, 0)
    return finish(got, residual)


def solution(mesh):
    fine = Mesh(mesh.devices.reshape(8, 2, 4, 2, 2), CTX + TP)
    return jax.shard_map(
        on_device,
        mesh=fine,
        in_specs=(P(CTX, TP), P(CTX, TP), P(CTX, TP), P(None, CTX), P(), P(TP, CTX), P(CTX + TP, None)),
        out_specs=P(CTX + TP, None),
        check_vma=False,
    )
```

```python
import functools
import math

import jax
import jax.numpy as jnp
from jax import lax
from jax.experimental import pallas as pl
from jax.experimental.pallas import tpu as pltpu
from jax.sharding import Mesh, PartitionSpec as P


HD = 128
theta_base = 1000000.0

CTX = ("z", "xh", "y")
TP = ("xl", "c")
XRING = ("xh", "xl")

TOK = 512
HEADS = 8
PIECE = 64
CHUNKS = 2
TQ = TOK // CHUNKS
BACK = 4
NEG = -1e30
EXP2_SCALE = math.log2(math.e) / math.sqrt(HD)


def from_behind(block, distance):
    size = math.prod(lax.axis_size(a) for a in CTX)
    route = [(i - distance, i) for i in range(distance, size)]
    return lax.ppermute(block, CTX, route)


def rotary_tables(positions):
    half_dim = HD // 2
    freq_index = jnp.arange(half_dim)
    inv_freq = theta_base ** (-2.0 * freq_index.astype(jnp.float32) / HD)
    first_end = HD // 8
    second_end = first_end + 3 * HD // 16
    place = positions.astype(jnp.float32)
    chosen = jnp.where(
        freq_index[None, :] < first_end,
        place[0][:, None],
        jnp.where(freq_index[None, :] < second_end, place[1][:, None], place[2][:, None]),
    )
    angle = chosen * inv_freq[None, :]
    cosine, sine = jnp.cos(angle), jnp.sin(angle)
    return jnp.concatenate([cosine, cosine], 1), jnp.concatenate([-sine, sine], 1)


def dot_nt(a, b):
    return lax.dot_general(a, b, (((1,), (1,)), ((), ())), preferred_element_type=jnp.float32)


def values_and_ones(value):
    return jnp.concatenate([value, jnp.ones_like(value)], axis=1)


def first_step(h, key, val, bias, rq_ref, m_ref, acc_ref):
    score = dot_nt(rq_ref[h], key) + bias
    peak = jnp.max(score, axis=1, keepdims=True)
    prob = jnp.exp2((score - peak) * EXP2_SCALE)
    m_ref[h] = jnp.broadcast_to(peak, (score.shape[0], HD))
    acc_ref[h] = jnp.dot(prob.astype(jnp.bfloat16), val, preferred_element_type=jnp.float32)


def next_step(h, key, val, bias, rq_ref, m_ref, acc_ref):
    score = dot_nt(rq_ref[h], key) + bias
    old = m_ref[h]
    new = jnp.maximum(old, jnp.broadcast_to(jnp.max(score, axis=1, keepdims=True), old.shape))
    keep = jnp.exp2((old - new) * EXP2_SCALE)
    wide = jnp.concatenate([new] * (score.shape[1] // HD), axis=1)
    prob = jnp.exp2((score - wide) * EXP2_SCALE)
    m_ref[h] = new
    acc_ref[h] = acc_ref[h] * jnp.concatenate([keep, keep], axis=1) + jnp.dot(
        prob.astype(jnp.bfloat16), val, preferred_element_type=jnp.float32
    )


def chunk_rows(i):
    return [pl.ds(b * 2 * PIECE + i * PIECE, PIECE) for b in range(TOK // (2 * PIECE))]


SMEM = pl.BlockSpec(memory_space=pltpu.SMEM)


def whole(shape):
    return pl.BlockSpec(shape, lambda n: (0,) * len(shape))


def attend_kernel(i, seg_s, qseg_ref, kseg_ref, q_ref, cos_ref, sin_ref, kv0, kv1, kv2, kv3, kv4, out_ref, rq_ref, m_ref, acc_ref):
    rows = chunk_rows(i)
    cosine = jnp.concatenate([cos_ref[r, :] for r in rows], axis=0)
    sine = jnp.concatenate([sin_ref[r, :] for r in rows], axis=0)
    for h in range(HEADS):
        x = jnp.concatenate([q_ref[r, h * HD : (h + 1) * HD] for r in rows], axis=0)
        x = x.astype(jnp.float32)
        rq_ref[h] = (x * cosine + pltpu.roll(x, HD // 2, 1) * sine).astype(jnp.bfloat16)
    qseg = jnp.concatenate([qseg_ref[r, :] for r in rows], axis=0)
    qseg = jnp.concatenate([qseg] * (TOK // HD), axis=1)
    row = lax.broadcasted_iota(jnp.int32, (TQ, TOK), 0)
    col = lax.broadcasted_iota(jnp.int32, (TQ, TOK), 1)
    token = (row // PIECE) * (2 * PIECE) + i * PIECE + row % PIECE
    bias = jnp.where((qseg == kseg_ref[BACK : BACK + 1, :]) & (col <= token), 0.0, NEG)
    for h in range(HEADS):
        first_step(h, kv0[:, :HD], values_and_ones(kv0[:, HD:]), bias, rq_ref, m_ref, acc_ref)
    for b, kv in enumerate((kv4, kv3, kv2, kv1)):

        @pl.when(seg_s[b * TOK + TOK - 1] == seg_s[BACK * TOK + i * PIECE])
        def _():
            bias = jnp.where(qseg == kseg_ref[b : b + 1, :], 0.0, NEG)
            for h in range(HEADS):
                next_step(h, kv[:, :HD], values_and_ones(kv[:, HD:]), bias, rq_ref, m_ref, acc_ref)

    for h in range(HEADS):
        full = acc_ref[h]
        out_ref[:, h * HD : (h + 1) * HD] = (full[:, :HD] / full[:, HD:]).astype(jnp.bfloat16)


def attend(i, seg, *blocks):
    return pl.pallas_call(
        functools.partial(attend_kernel, i),
        out_shape=jax.ShapeDtypeStruct((TQ, HEADS * HD), jnp.bfloat16),
        grid=(1,),
        in_specs=[SMEM] + [whole(b.shape) for b in blocks],
        out_specs=whole((TQ, HEADS * HD)),
        scratch_shapes=[
            pltpu.VMEM((HEADS, TQ, HD), jnp.bfloat16),
            pltpu.VMEM((HEADS, TQ, HD), jnp.float32),
            pltpu.VMEM((HEADS, TQ, 2 * HD), jnp.float32),
        ],
        compiler_params=pltpu.CompilerParams(vmem_limit_bytes=24 << 20),
    )(seg, *blocks)


def project_kernel(at, own_ref, oth_ref, w_ref, out_ref):
    places = [at[1] ^ (2 * far + core) for core in range(2) for far in range(2)]
    w = jnp.concatenate(
        [jnp.concatenate([w_ref[0, p], w_ref[1, p]], axis=1) for p in places], axis=0
    )
    a = jnp.concatenate([own_ref[0], own_ref[1], oth_ref[0], oth_ref[1]], axis=1)
    acc = jnp.dot(a, w, preferred_element_type=jnp.float32)
    for e in range(2):
        for i in range(CHUNKS):
            first = (e * CHUNKS + i) * TQ
            block = acc[first : first + TQ].astype(jnp.bfloat16)
            s = at[0] if e == 0 else 1 - at[0]
            out_ref[s, :, i] = block.reshape(TQ // PIECE, PIECE, 2 * HD)


def project(at, own, oth, weight):
    steps = weight.shape[0] // 2
    rows = (2, TQ // PIECE, CHUNKS, PIECE)
    return pl.pallas_call(
        project_kernel,
        out_shape=jax.ShapeDtypeStruct(rows + (2 * steps * HD,), jnp.bfloat16),
        grid=(steps,),
        in_specs=[SMEM]
        + [pl.BlockSpec(memory_space=pltpu.VMEM)] * 2
        + [pl.BlockSpec((2,) + weight.shape[1:], lambda n: (n, 0, 0, 0))],
        out_specs=pl.BlockSpec(rows + (2 * HD,), lambda n: (0, 0, 0, 0, n)),
        compiler_params=pltpu.CompilerParams(vmem_limit_bytes=36 << 20),
        name="project",
    )(at, own, oth, weight)


def finish_kernel(got_ref, res_ref, out_ref):
    srcs, zs = got_ref.shape[0], got_ref.shape[2] // HD
    for z in range(zs):
        for s in range(srcs):
            cols = pl.ds((z * srcs + s) * HD, HD)
            out_ref[:, cols] = (
                got_ref[s, :, z * HD : (z + 1) * HD].astype(jnp.float32)
                + res_ref[:, cols].astype(jnp.float32)
            ).astype(jnp.bfloat16)


def finish(got, residual):
    srcs, rows, cols = got.shape
    step = 64
    wide = pl.BlockSpec((step, srcs * cols), lambda r: (r, 0))
    return pl.pallas_call(
        finish_kernel,
        out_shape=jax.ShapeDtypeStruct(residual.shape, jnp.bfloat16),
        grid=(rows // step,),
        in_specs=[pl.BlockSpec((srcs, step, cols), lambda r: (0, r, 0)), wide],
        out_specs=wide,
        compiler_params=pltpu.CompilerParams(vmem_limit_bytes=16 << 20),
        name="finish",
    )(got, residual)


def swap4(block, axes, j):
    return lax.ppermute(block, axes, [(r, r ^ j) for r in range(4)])


def gather4(i, block, axes):
    j1 = swap4(block, axes, 1)
    j3 = swap4(block, axes, 3)
    j2 = swap4(*((j3, axes, 1) if i == 0 else (j1, axes, 3)))
    return block, j1, j2, j3


def other_core(block):
    return lax.ppermute(block, "c", [(0, 1), (1, 0)])


def on_device(queries, keys, values, positions, segment_ids, out_weight, residual):
    swap = [(y * 4 + t, t * 4 + y) for y in range(4) for t in range(4)]
    mine = lax.ppermute(out_weight, ("y",) + TP, swap)
    weight = lax.all_gather(mine, ("z", "y"), axis=0).reshape((8, 4) + mine.shape)

    cosine, sine = rotary_tables(positions)
    k32 = keys.astype(jnp.float32)
    flipped = jnp.concatenate([k32[:, HD // 2 :], k32[:, : HD // 2]], axis=1)
    rot_k = (k32 * cosine + flipped * sine).astype(jnp.bfloat16)
    kv = jnp.concatenate([rot_k, values], axis=1)
    behind = [from_behind(kv, d) for d in range(1, BACK + 1)]

    my_start = lax.axis_index(CTX) * TOK
    padded = jnp.concatenate([jnp.full((BACK * TOK,), -1, jnp.int32), segment_ids])
    seg = lax.dynamic_slice_in_dim(padded, my_start, (BACK + 1) * TOK, 0)
    qseg = jnp.broadcast_to(seg[BACK * TOK :, None], (TOK, HD))
    kseg = jnp.pad(seg.reshape(BACK + 1, TOK), ((0, 3), (0, 0)))

    near, far = [[], []], [[], []]
    for i in range(CHUNKS):
        own = attend(i, seg, qseg, kseg, queries, cosine, sine, kv, *behind)
        own, j1, j2, j3 = gather4(i, own, XRING)
        for side, blocks in ((near, (own, j2)), (far, (j1, j3))):
            for rows, block in zip(side, blocks):
                rows.append(block)
    own = jnp.concatenate([b for side in (near, far) for rows in side for b in rows], axis=0)
    own = own.reshape(2, 2 * TOK, HEADS * HD)
    oth = other_core(own)

    xh, xl, c = (lax.axis_index(a).astype(jnp.int32) for a in ("xh", "xl", "c"))
    at = jnp.stack([xh, 2 * xl + c])
    out = project(at, own, oth, weight)
    out = out.reshape(8, CHUNKS * PIECE, out.shape[-1])
    got = lax.all_to_all(out, XRING + ("c",), 0, 0)
    return finish(got, residual)


def solution(mesh):
    fine = Mesh(mesh.devices.reshape(8, 2, 4, 2, 2), CTX + TP)
    return jax.shard_map(
        on_device,
        mesh=fine,
        in_specs=(P(CTX, TP), P(CTX, TP), P(CTX, TP), P(None, CTX), P(), P(TP, CTX), P(CTX + TP, None)),
        out_specs=P(CTX + TP, None),
        check_vma=False,
    )
```
